128 devices in a mesh: row: 8 (over z_lo, y), col: 16 (over x, z_hi, core).
Axes of the slice: x: 4, y: 4, z: 4 (z_hi: 2, z_lo: 2; z = z_hi * 2 + z_lo), core: 2. Of those that a mesh axis runs over, the one named last changes fastest.
Arguments:
- panel: bfloat16 [524288, 256], P(('row', 'col')), may hold values from -6 to 6
- row_basis: bfloat16 [524288, 16], P('row'), may hold values from -1.5 to 1.5
- col_basis: bfloat16 [524288, 16], P(('row', 'col')), may hold values from -0.375 to 0.375
- near_blocks: bfloat16 [2048, 9, 256, 256], P(('row', 'col')), may hold values from -0.125 to 0.125
- couplings: bfloat16 [8, 16, 512, 16, 16], P('row', 'col'), may hold values from -0.375 to 0.375
- blk_rows: int32 [8, 16, 512], P('row', 'col'), may hold values from 0 to 255
- blk_cols: int32 [8, 16, 512], P('row', 'col'), may hold values from 0 to 127
- blk_count: int32 [8, 16], P('row', 'col'), may hold values from 64 to 512, as said below
Outputs:
- product: bfloat16 [524288, 256], P(('row', 'col'))
The draws below stay inside these ranges and needn't reach their ends.
Inputs may be any that keep to these rules, and one draw needn't show every extreme that they name: `blk_count`: slots at or past a device's count hold in-range indices and are not part of the matrix; in every draw some device holds 512 live slots.
All inputs are finite; a program needn't handle non-finite values.
Results may differ from the reference program's by a relative error of at most 0.0052.
Values may be sent and summed in bfloat16 or wider, within the bound.
No kernel may reach another device: no remote copies, remote signals or barrier semaphores. Data moves between devices by JAX's collectives and lax.ppermute only.
A program may use at most 192 MiB of HBM per device.

```python
import jax
import jax.numpy as jnp
from jax import lax

LEAF = 256
R = 16
NRHS = 256
HALF = 4
FAR_PER_CL = 32
CPD = 16
NEAR = 9
FAR_DEV = 512
NCL = 2048
NPTS = 524288
N_ROW = 8
N_COL = 16


def draw_blk_count(key, part):
    first_key, second_key = jax.random.split(jax.random.fold_in(key, 17))
    raw_level = jax.random.randint(first_key, (N_ROW * N_COL,), 0, 64)
    lowest = FAR_DEV // 8
    counts = lowest + (FAR_DEV - lowest) * raw_level * raw_level // (63 * 63)
    fullest = jax.random.randint(second_key, (), 0, N_ROW * N_COL)
    counts = jnp.where(jnp.arange(N_ROW * N_COL) == fullest, FAR_DEV, counts)
    return counts.reshape(N_ROW, N_COL).astype(jnp.int32)


def set_ends(entries, key, low, largest):
    extent = entries.shape
    spot = [jax.random.randint(jax.random.fold_in(key, axis), (), 0, extent[axis]) for axis in range(len(extent))]
    entries = entries.at[tuple(spot)].set(low)
    longest = extent.index(max(extent))
    spot[longest] = (spot[longest] + 1) % extent[longest]
    return entries.at[tuple(spot)].set(largest)


def block_scale(rng, shape, shards, low, top_value):
    factor_of, own = 1.0, jax.random.fold_in(rng, 6)
    for axis_at, parts in shards:
        heights = jnp.exp(jax.random.uniform(jax.random.fold_in(own, axis_at), (parts,), jnp.float32, low / len(shards), top_value / len(shards)))
        factor_of = factor_of * jnp.repeat(heights, shape[axis_at] // parts).reshape([-1 if axis == axis_at else 1 for axis in range(len(shape))])
    return factor_of


def gaussian(key, shape, width, bound, pieces=(), held_as=jnp.bfloat16):
    values = jax.random.normal(key, shape, jnp.float32) * width
    if len(pieces) > 0:
        values = block_scale(key, shape, pieces, -0.22, 0.18) * values
    return jnp.clip(values, min=-bound, max=bound).astype(held_as)


def setup_inputs(seed: int = 0) -> dict:
    seeds = jax.random.split(jax.random.key(seed), 9)
    return {
        "panel": gaussian(seeds[0], (NPTS, NRHS), 1.0, 6.0, ((0, 128),)),
        "row_basis": gaussian(seeds[1], (NPTS, R), R ** -0.5, 1.5, ((0, 8),)),
        "col_basis": gaussian(seeds[2], (NPTS, R), LEAF ** -0.5, 0.375, ((0, 128),)),
        "near_blocks": gaussian(seeds[3], (NCL, NEAR, LEAF, LEAF), (NEAR * LEAF) ** -0.5, 0.125, ((0, 128),)),
        "couplings": gaussian(seeds[4], (N_ROW, N_COL, FAR_DEV, R, R), (R * FAR_PER_CL // 2) ** -0.5, 0.375, ((0, 8), (1, 16))),
        "blk_rows": set_ends(jax.random.randint(seeds[5], (N_ROW, N_COL, FAR_DEV), 0, N_COL * CPD), jax.random.fold_in(seeds[5], 1), 0, (N_COL * CPD) - 1).astype(jnp.int32),
        "blk_cols": set_ends(jax.random.randint(seeds[6], (N_ROW, N_COL, FAR_DEV), 0, N_ROW * CPD), jax.random.fold_in(seeds[6], 1), 0, (N_ROW * CPD) - 1).astype(jnp.int32),
        "blk_count": draw_blk_count(jax.random.fold_in(seeds[8], 71), 0),
    }


def reference(panel, row_basis, col_basis, near_blocks, couplings, blk_rows, blk_cols, blk_count):
    cluster_total = NPTS // LEAF
    highest = lax.Precision.HIGHEST
    clusters = panel.reshape(cluster_total, LEAF, NRHS).astype(jnp.float32)
    coeffs = jnp.einsum('kpr,kpn->krn', col_basis.reshape(cluster_total, LEAF, R).astype(jnp.float32), clusters, precision=highest).astype(jnp.bfloat16)
    owner_row = jnp.arange(N_ROW, dtype=jnp.int32)[:, None, None]
    owner_col = jnp.arange(N_COL, dtype=jnp.int32)[None, :, None]
    global_row = owner_row * (N_COL * CPD) + blk_rows
    global_col = ((blk_cols // CPD) * N_COL + owner_col) * CPD + blk_cols % CPD
    is_live = jnp.arange(FAR_DEV, dtype=jnp.int32)[None, None, :] < blk_count[:, :, None]
    slot_total = N_ROW * N_COL * FAR_DEV
    picked = coeffs[global_col.reshape(slot_total)].astype(jnp.float32)
    block_terms = jnp.einsum('bij,bjn->bin', couplings.reshape(slot_total, R, R).astype(jnp.float32), picked, precision=highest)
    block_terms = jnp.where(is_live.reshape(slot_total)[:, None, None], block_terms, jnp.float32(0.0))
    coupled = jax.ops.segment_sum(block_terms, global_row.reshape(slot_total), num_segments=cluster_total)
    far_field = jnp.einsum('kpr,krn->kpn', row_basis.reshape(cluster_total, LEAF, R).astype(jnp.float32), coupled, precision=highest)
    padded = jnp.pad(clusters, ((HALF, HALF), (0, 0), (0, 0)))
    near_field = jnp.zeros((cluster_total, LEAF, NRHS), jnp.float32)
    for offset in range(NEAR):
        near_field = near_field + jnp.einsum('kpq,kqn->kpn', near_blocks[:, offset].astype(jnp.float32), padded[offset:offset + cluster_total], precision=highest)
    return (near_field + far_field).reshape(NPTS, NRHS).astype(jnp.bfloat16)
```

```python
import functools

import jax
import jax.numpy as jnp
from jax import lax
from jax.experimental import pallas as pl
from jax.experimental.pallas import tpu as pltpu
from jax.sharding import Mesh, PartitionSpec as P

F32, BF16, I32 = jnp.float32, jnp.bfloat16, jnp.int32
ROW, COL = ("zl", "y"), ("x", "zh", "core")
NT = (((1,), (1,)), ((), ()))
TN = (((0,), (0,)), ((), ()))
VMEM = pl.BlockSpec(memory_space=pltpu.VMEM)
SMEM = pl.BlockSpec(memory_space=pltpu.SMEM)


def cost(flops, nbytes):
    return pl.CostEstimate(flops=flops, bytes_accessed=nbytes, transcendentals=0)


def params(mib):
    return pltpu.CompilerParams(vmem_limit_bytes=mib << 20)


def coeff_kernel(peers, leaf, rank, half, panel_ref, vt_ref, send_ref, head_ref, tail_ref):
    rows = panel_ref.shape[0]
    for k in range(rows // leaf):
        span = pl.ds(k * leaf, leaf)
        value = jnp.dot(vt_ref[:, span], panel_ref[span, :], preferred_element_type=F32).astype(BF16)
        for peer in range(peers):
            send_ref[peer, pl.ds(k * rank, rank), :] = value
    head_ref[...] = panel_ref[pl.ds(0, half * leaf), :]
    tail_ref[...] = panel_ref[pl.ds(rows - half * leaf, half * leaf), :]


def prep_kernel(per_dev, rank, groups, info_ref, rows_ref, cols_ref, x_ref, ct_ref, table_ref):
    slots = rows_ref.shape[1]
    count, core = info_ref[0], info_ref[1]
    lane = lax.broadcasted_iota(I32, (1, slots), 1)
    live = lane < count
    rows = rows_ref[...]
    dest, local = rows // per_dev, rows % per_dev
    other = jnp.where(dest % 2 == core, 0, 1)
    row_key = other * (groups // 2) + (dest // 2) * per_dev + local
    key = jnp.where(live, row_key, groups) * slots + lane
    down = lax.broadcasted_iota(I32, (slots, slots), 0)
    across = lax.broadcasted_iota(I32, (slots, slots), 1)
    key_down = jnp.sum(jnp.where(down == across, key, 0), axis=1, keepdims=True)
    place = jnp.sum((key_down < key).astype(I32), axis=0, keepdims=True)
    place = jnp.where(live, place, -1)
    pick = (down == place).astype(F32).astype(BF16)
    value = lax.dot_general(pick, x_ref[...], NT, preferred_element_type=F32)
    width = value.shape[1]
    k_of = lax.broadcasted_iota(I32, value.shape, 0)
    i_of = lax.broadcasted_iota(I32, value.shape, 1) // rank
    step = 1
    while step < rank:
        k_bit, i_bit = (k_of // step) % 2, (i_of // step) % 2
        ahead = pltpu.roll(pltpu.roll(value, slots - step, 0), step * rank, 1)
        behind = pltpu.roll(pltpu.roll(value, step, 0), width - step * rank, 1)
        value = jnp.where(k_bit == i_bit, value, jnp.where(k_bit == 0, ahead, behind))
        step *= 2
    ct_ref[...] = value.astype(BF16)
    top = jnp.max(jnp.where(live, row_key, 0))
    pair = jnp.concatenate([cols_ref[...], row_key] + [jnp.zeros_like(row_key)] * 6, axis=0)
    table = lax.dot_general(pair.astype(F32).astype(BF16), pick, NT, preferred_element_type=F32).astype(I32)
    which = lax.broadcasted_iota(I32, table.shape, 0)
    past = lax.broadcasted_iota(I32, table.shape, 1) >= count
    table_ref[...] = jnp.where(past & (which == 1), top, table)


def block_kernel(rank, tile, unroll, table_ref, ct_ref, g_ref, own_ref, other_ref, out_ref):
    slots = table_ref.shape[1]
    cols = g_ref.shape[1]
    out_ref[...] = jnp.zeros_like(out_ref)
    width = tile * rank
    group = lax.broadcasted_iota(I32, (rank, width), 1) // rank
    masks = [(group == k).astype(F32).astype(BF16) for k in range(tile)]
    halves = ct_ref.shape[1] // width

    def body(step, carry):
        acc, last = carry
        for u in range(unroll):
            for h in range(halves):
                base = (step * unroll + u) * tile * halves + h * tile
                ct = ct_ref[pl.ds(pl.multiple_of((step * unroll + u) * rank, rank), rank), h * width : (h + 1) * width]
                lhs = jnp.concatenate([ct * m for m in masks], axis=0)
                rhs = jnp.concatenate(
                    [
                        g_ref[pl.ds(pl.multiple_of(table_ref[0, base + k] * rank, rank), rank), :]
                        for k in range(tile)
                    ],
                    axis=0,
                )
                terms = jnp.dot(lhs, rhs, preferred_element_type=F32)
                for k in range(tile):
                    row = table_ref[1, base + k]
                    term = terms[k * rank : (k + 1) * rank, :]
                    acc = term + jnp.where(row == last, acc, 0.0)
                    last = row
                    out_ref[pl.ds(pl.multiple_of(row * rank, rank), rank), :] = acc.astype(BF16)
        return acc, last

    steps = slots // (tile * halves * unroll)
    lax.fori_loop(0, steps, body, (jnp.zeros((rank, cols), F32), jnp.int32(-1)))
    size = own_ref.shape[0]
    own_ref[...] = out_ref[pl.ds(0, size), :]
    other_ref[...] = out_ref[pl.ds(size, size), :]


def pair_kernel(a_ref, b_ref, out_ref):
    out_ref[...] = (a_ref[...].astype(F32) + b_ref[...].astype(F32)).astype(BF16)


def near_kernel(half, leaf, nb_ref, panel_ref, low_ref, high_ref, out_ref, window):
    k = pl.program_id(0)
    rows, edge = panel_ref.shape[0], half * leaf

    @pl.when(k == 0)
    def _():
        window[pl.ds(0, edge), :] = low_ref[...]
        window[pl.ds(edge, rows), :] = panel_ref[...]
        window[pl.ds(edge + rows, edge), :] = high_ref[...]

    total = None
    for o in range(nb_ref.shape[1]):
        rhs = window[pl.ds(pl.multiple_of((k + o) * leaf, leaf), leaf), :]
        term = jnp.dot(nb_ref[0, o], rhs, preferred_element_type=F32)
        total = term if total is None else total + term
    out_ref[...] = total


def final_kernel(place_ref, parts_ref, ut_ref, near_ref, out_ref):
    coupled = parts_ref[0].astype(F32)
    for p in range(1, parts_ref.shape[0]):
        coupled = coupled + parts_ref[p].astype(F32)
    high = coupled.astype(BF16)
    low = (coupled - high.astype(F32)).astype(BF16)
    ut = ut_ref[...]
    far = lax.dot_general(
        jnp.concatenate([ut, ut], axis=0), jnp.concatenate([high, low], axis=0), TN, preferred_element_type=F32
    )
    out_ref[...] = (near_ref[...] + far).astype(BF16)


def on_device(panel, row_basis, col_basis, near_blocks, couplings, blk_rows, blk_cols, blk_count):
    rows, cols = panel.shape
    clusters, near_count, leaf, _ = near_blocks.shape
    rank, slots = col_basis.shape[1], couplings.shape[2]
    half = near_count // 2
    row_peers, col_peers = lax.axis_size(ROW), lax.axis_size(COL)
    groups = col_peers * clusters
    core = lax.axis_index("core")

    send, head, tail = pl.pallas_call(
        functools.partial(coeff_kernel, row_peers, leaf, rank, half),
        out_shape=(
            jax.ShapeDtypeStruct((row_peers, clusters * rank, cols), BF16),
            jax.ShapeDtypeStruct((half * leaf, cols), BF16),
            jax.ShapeDtypeStruct((half * leaf, cols), BF16),
        ),
        in_specs=[VMEM, VMEM],
        out_specs=(VMEM, VMEM, VMEM),
        compiler_params=params(16),
        cost_estimate=cost(2 * rows * rank * cols, 5 << 20),
        name="coeffs",
    )(panel, col_basis.T)
    gathered = lax.all_to_all(send, ROW, 0, 0, tiled=True)

    every = ROW + COL
    peers = lax.axis_size(every)
    up = [(i, i + 1) for i in range(peers - 1)]
    low = lax.ppermute(tail, every, up)
    high = lax.ppermute(head, every, [(b, a) for a, b in up])

    info = jnp.stack([blk_count.reshape(()), core.astype(I32)])
    x = jnp.transpose(couplings.reshape(slots, rank, rank), (1, 2, 0)).reshape(rank * rank, slots)
    ct, table = pl.pallas_call(
        functools.partial(prep_kernel, clusters, rank, groups),
        out_shape=(jax.ShapeDtypeStruct((slots, rank * rank), BF16), jax.ShapeDtypeStruct((8, slots), I32)),
        in_specs=[SMEM, VMEM, VMEM, VMEM],
        out_specs=(VMEM, VMEM),
        compiler_params=params(24),
        cost_estimate=cost(2 * slots * slots * rank * rank, 1 << 20),
        name="prep",
    )(info, blk_rows.reshape(1, slots), blk_cols.reshape(1, slots), x)

    mine, theirs = pl.pallas_call(
        functools.partial(block_kernel, rank, 128 // rank, 4),
        out_shape=[jax.ShapeDtypeStruct((groups // 2 * rank, cols), BF16)] * 2,
        in_specs=[SMEM, VMEM, VMEM],
        out_specs=[VMEM, VMEM],
        scratch_shapes=[pltpu.VMEM((groups * rank, cols), BF16)],
        compiler_params=params(24),
        cost_estimate=cost(2 * slots * rank * 128 * cols, 4 << 20),
        name="blocks",
    )(table, ct, gathered.reshape(row_peers * clusters * rank, cols))

    swapped = lax.ppermute(theirs, "core", [(0, 1), (1, 0)])
    summed = pl.pallas_call(
        pair_kernel,
        out_shape=jax.ShapeDtypeStruct(mine.shape, BF16),
        in_specs=[VMEM, VMEM],
        out_specs=VMEM,
        compiler_params=params(16),
        cost_estimate=cost(mine.size, 3 << 20),
        name="pair",
    )(mine, swapped)
    parts = lax.all_to_all(
        summed.reshape(col_peers // 2, clusters * rank, cols), ("x", "zh"), 0, 0, tiled=True
    )

    near = pl.pallas_call(
        functools.partial(near_kernel, half, leaf),
        out_shape=jax.ShapeDtypeStruct((rows, cols), F32),
        grid=(clusters,),
        in_specs=[
            pl.BlockSpec((1, near_count, leaf, leaf), lambda k: (k, 0, 0, 0)),
            pl.BlockSpec((rows, cols), lambda k: (0, 0)),
            pl.BlockSpec((half * leaf, cols), lambda k: (0, 0)),
            pl.BlockSpec((half * leaf, cols), lambda k: (0, 0)),
        ],
        out_specs=pl.BlockSpec((leaf, cols), lambda k: (k, 0)),
        scratch_shapes=[pltpu.VMEM((rows + 2 * half * leaf, cols), BF16)],
        compiler_params=params(32),
        cost_estimate=cost(2 * clusters * near_count * leaf * leaf * cols, 28 << 20),
        name="near",
    )(near_blocks, panel, low, high)

    place = lax.axis_index(COL).astype(I32).reshape(1)
    return pl.pallas_call(
        final_kernel,
        out_shape=jax.ShapeDtypeStruct((rows, cols), BF16),
        grid_spec=pltpu.PrefetchScalarGridSpec(
            num_scalar_prefetch=1,
            grid=(clusters,),
            in_specs=[
                pl.BlockSpec((col_peers // 2, rank, cols), lambda k, at: (0, k, 0)),
                pl.BlockSpec((rank, leaf), lambda k, at: (0, at[0] * clusters + k)),
                pl.BlockSpec((leaf, cols), lambda k, at: (k, 0)),
            ],
            out_specs=pl.BlockSpec((leaf, cols), lambda k, at: (k, 0)),
        ),
        compiler_params=params(16),
        cost_estimate=cost(4 * rows * rank * cols, 8 << 20),
        name="final",
    )(place, parts, row_basis.T, near)


def solution(mesh):
    devices = mesh.devices.reshape(2, 4, 4, 2, 2)
    fine = Mesh(devices, ("zl", "y", "x", "zh", "core"))
    placed = (
        P((*ROW, *COL), None),
        P(ROW, None),
        P((*ROW, *COL), None),
        P((*ROW, *COL), None, None, None),
        P(ROW, COL, None, None, None),
        P(ROW, COL, None),
        P(ROW, COL, None),
        P(ROW, COL),
    )
    return jax.shard_map(
        on_device, mesh=fine, in_specs=placed, out_specs=P((*ROW, *COL), None), check_vma=False
    )
```

```python
import functools

import jax
import jax.numpy as jnp
from jax import lax
from jax.experimental import pallas as pl
from jax.experimental.pallas import tpu as pltpu
from jax.sharding import Mesh, PartitionSpec as P


F32, BF16, I32 = jnp.float32, jnp.bfloat16, jnp.int32
ROW, COL = ("zl", "y"), ("x", "zh", "core")
NT = (((1,), (1,)), ((), ()))
TN = (((0,), (0,)), ((), ()))
VMEM = pl.BlockSpec(memory_space=pltpu.VMEM)
SMEM = pl.BlockSpec(memory_space=pltpu.SMEM)


def cost(flops, nbytes):
    return pl.CostEstimate(flops=flops, bytes_accessed=nbytes, transcendentals=0)


def params(mib):
    return pltpu.CompilerParams(vmem_limit_bytes=mib << 20)


def coeff_kernel(peers, leaf, rank, panel_ref, vt_ref, send_ref, head_ref, tail_ref):
    step = pl.program_id(0)
    for k in range(panel_ref.shape[0] // leaf):
        span = pl.ds(k * leaf, leaf)
        value = jnp.dot(vt_ref[:, span], panel_ref[span, :], preferred_element_type=F32).astype(BF16)
        for peer in range(peers):
            send_ref[peer, pl.ds(k * rank, rank), :] = value

    @pl.when(step == 0)
    def _():
        head_ref[...] = panel_ref[...]

    @pl.when(step == pl.num_programs(0) - 1)
    def _():
        tail_ref[...] = panel_ref[...]


def prep_kernel(per_dev, rank, groups, info_ref, rows_ref, cols_ref, x_ref, ct_ref, table_ref):
    slots = rows_ref.shape[1]
    count, core = info_ref[0], info_ref[1]
    lane = lax.broadcasted_iota(I32, (1, slots), 1)
    live = lane < count
    rows = rows_ref[...]
    dest, local = rows // per_dev, rows % per_dev
    other = jnp.where(dest % 2 == core, 0, 1)
    row_key = other * (groups // 2) + (dest // 2) * per_dev + local
    key = jnp.where(live, row_key, groups) * slots + lane
    down = lax.broadcasted_iota(I32, (slots, slots), 0)
    across = lax.broadcasted_iota(I32, (slots, slots), 1)
    key_down = jnp.sum(jnp.where(down == across, key, 0), axis=1, keepdims=True)
    place = jnp.sum((key_down < key).astype(I32), axis=0, keepdims=True)
    place = jnp.where(live, place, -1)
    pick = (down == place).astype(F32).astype(BF16)
    value = lax.dot_general(pick, x_ref[...], NT, preferred_element_type=F32)
    width = value.shape[1]
    k_of = lax.broadcasted_iota(I32, value.shape, 0)
    i_of = lax.broadcasted_iota(I32, value.shape, 1) // rank
    step = 1
    while step < rank:
        k_bit, i_bit = (k_of // step) % 2, (i_of // step) % 2
        ahead = pltpu.roll(pltpu.roll(value, slots - step, 0), step * rank, 1)
        behind = pltpu.roll(pltpu.roll(value, step, 0), width - step * rank, 1)
        value = jnp.where(k_bit == i_bit, value, jnp.where(k_bit == 0, ahead, behind))
        step *= 2
    ct_ref[...] = value.astype(BF16)
    top = jnp.max(jnp.where(live, row_key, 0))
    pair = jnp.concatenate([cols_ref[...], row_key] + [jnp.zeros_like(row_key)] * 6, axis=0)
    table = lax.dot_general(pair.astype(F32).astype(BF16), pick, NT, preferred_element_type=F32).astype(I32)
    which = lax.broadcasted_iota(I32, table.shape, 0)
    past = lax.broadcasted_iota(I32, table.shape, 1) >= count
    table_ref[...] = jnp.where(past & (which == 1), top, table)


def block_kernel(rank, tile, unroll, table_ref, ct_ref, g_ref, own_ref, other_ref, out_ref):
    slots = table_ref.shape[1]
    cols = g_ref.shape[1]
    out_ref[...] = jnp.zeros_like(out_ref)
    width = tile * rank
    group = lax.broadcasted_iota(I32, (rank, width), 1) // rank
    masks = [(group == k).astype(F32).astype(BF16) for k in range(tile)]
    halves = ct_ref.shape[1] // width

    def body(step, carry):
        acc, last = carry
        for u in range(unroll):
            for h in range(halves):
                base = (step * unroll + u) * tile * halves + h * tile
                ct = ct_ref[pl.ds(pl.multiple_of((step * unroll + u) * rank, rank), rank), h * width : (h + 1) * width]
                lhs = jnp.concatenate([ct * m for m in masks], axis=0)
                rhs = jnp.concatenate(
                    [
                        g_ref[pl.ds(pl.multiple_of(table_ref[0, base + k] * rank, rank), rank), :]
                        for k in range(tile)
                    ],
                    axis=0,
                )
                terms = jnp.dot(lhs, rhs, preferred_element_type=F32)
                for k in range(tile):
                    row = table_ref[1, base + k]
                    term = terms[k * rank : (k + 1) * rank, :]
                    acc = term + jnp.where(row == last, acc, 0.0)
                    last = row
                    out_ref[pl.ds(pl.multiple_of(row * rank, rank), rank), :] = acc.astype(BF16)
        return acc, last

    steps = slots // (tile * halves * unroll)
    lax.fori_loop(0, steps, body, (jnp.zeros((rank, cols), F32), jnp.int32(-1)))
    size = own_ref.shape[0]
    own_ref[...] = out_ref[pl.ds(0, size), :]
    other_ref[...] = out_ref[pl.ds(size, size), :]


def pair_kernel(a_ref, b_ref, out_ref):
    out_ref[...] = (a_ref[...].astype(F32) + b_ref[...].astype(F32)).astype(BF16)


def near_kernel(half, leaf, nb_ref, panel_ref, low_ref, high_ref, out_ref, window):
    step = pl.program_id(0)
    rows, edge = panel_ref.shape[0], half * leaf
    held, near_count = nb_ref.shape[:2]

    @pl.when(step == 0)
    def _():
        window[pl.ds(0, edge), :] = low_ref[...]
        window[pl.ds(edge, rows), :] = panel_ref[...]
        window[pl.ds(edge + rows, edge), :] = high_ref[...]

    for c in range(held):
        lhs = jnp.concatenate([nb_ref[c, o] for o in range(near_count)], axis=1)
        rhs = window[pl.ds(pl.multiple_of((step * held + c) * leaf, leaf), near_count * leaf), :]
        out_ref[pl.ds(c * leaf, leaf), :] = jnp.dot(lhs, rhs, preferred_element_type=F32)


def final_kernel(rank, leaf, place_ref, parts_ref, ut_ref, near_ref, out_ref):
    for k in range(near_ref.shape[0] // leaf):
        span, ranks = pl.ds(k * leaf, leaf), pl.ds(k * rank, rank)
        coupled = parts_ref[0, ranks, :].astype(F32)
        for p in range(1, parts_ref.shape[0]):
            coupled = coupled + parts_ref[p, ranks, :].astype(F32)
        high = coupled.astype(BF16)
        low = (coupled - high.astype(F32)).astype(BF16)
        ut = ut_ref[:, span]
        far = lax.dot_general(
            jnp.concatenate([ut, ut], axis=0), jnp.concatenate([high, low], axis=0), TN, preferred_element_type=F32
        )
        out_ref[span, :] = (near_ref[span, :] + far).astype(BF16)


def on_device(panel, row_basis, col_basis, near_blocks, couplings, blk_rows, blk_cols, blk_count):
    rows, cols = panel.shape
    clusters, near_count, leaf, _ = near_blocks.shape
    rank, slots = col_basis.shape[1], couplings.shape[2]
    half = near_count // 2
    row_peers, col_peers = lax.axis_size(ROW), lax.axis_size(COL)
    groups = col_peers * clusters
    core = lax.axis_index("core")

    edge = half * leaf
    send, head, tail = pl.pallas_call(
        functools.partial(coeff_kernel, row_peers, leaf, rank),
        out_shape=(
            jax.ShapeDtypeStruct((row_peers, clusters * rank, cols), BF16),
            jax.ShapeDtypeStruct((edge, cols), BF16),
            jax.ShapeDtypeStruct((edge, cols), BF16),
        ),
        grid=(rows // edge,),
        in_specs=[pl.BlockSpec((edge, cols), lambda k: (k, 0)), pl.BlockSpec((rank, edge), lambda k: (0, k))],
        out_specs=(
            pl.BlockSpec((row_peers, half * rank, cols), lambda k: (0, k, 0)),
            pl.BlockSpec((edge, cols), lambda k: (0, 0)),
            pl.BlockSpec((edge, cols), lambda k: (0, 0)),
        ),
        compiler_params=params(60),
        cost_estimate=cost(2 * rows * rank * cols, 5 << 20),
        name="coeffs",
    )(panel, col_basis.T)
    gathered = lax.all_to_all(send, ROW, 0, 0, tiled=True)

    every = ROW + COL
    peers = lax.axis_size(every)
    up = [(i, i + 1) for i in range(peers - 1)]
    low = lax.ppermute(tail, every, up)
    high = lax.ppermute(head, every, [(b, a) for a, b in up])

    info = jnp.stack([blk_count.reshape(()), core.astype(I32)])
    x = jnp.transpose(couplings.reshape(slots, rank, rank), (1, 2, 0)).reshape(rank * rank, slots)
    prep = pl.pallas_call(
        functools.partial(prep_kernel, clusters, rank, groups),
        out_shape=(jax.ShapeDtypeStruct((slots, rank * rank), BF16), jax.ShapeDtypeStruct((8, slots), I32)),
        in_specs=[SMEM, VMEM, VMEM, VMEM],
        out_specs=(VMEM, VMEM),
        compiler_params=params(24),
        cost_estimate=cost(2 * slots * slots * rank * rank, 1 << 20),
        name="prep",
    )
    ct, table = prep(info, blk_rows.reshape(1, slots), blk_cols.reshape(1, slots), x)

    mine, theirs = pl.pallas_call(
        functools.partial(block_kernel, rank, 128 // rank, 4),
        out_shape=[jax.ShapeDtypeStruct((groups // 2 * rank, cols), BF16)] * 2,
        in_specs=[SMEM, VMEM, VMEM],
        out_specs=[VMEM, VMEM],
        scratch_shapes=[pltpu.VMEM((groups * rank, cols), BF16)],
        compiler_params=params(24),
        cost_estimate=cost(2 * slots * rank * 128 * cols, 4 << 20),
        name="blocks",
    )(table, ct, gathered.reshape(row_peers * clusters * rank, cols))

    swapped = lax.ppermute(theirs, "core", [(0, 1), (1, 0)])
    summed = pl.pallas_call(
        pair_kernel,
        out_shape=jax.ShapeDtypeStruct(mine.shape, BF16),
        in_specs=[VMEM, VMEM],
        out_specs=VMEM,
        compiler_params=params(16),
        cost_estimate=cost(mine.size, 3 << 20),
        name="pair",
    )(mine, swapped)
    parts = lax.all_to_all(
        summed.reshape(col_peers // 2, clusters * rank, cols), ("x", "zh"), 0, 0, tiled=True
    )

    held = 2
    near = pl.pallas_call(
        functools.partial(near_kernel, half, leaf),
        out_shape=jax.ShapeDtypeStruct((rows, cols), F32),
        grid=(clusters // held,),
        in_specs=[
            pl.BlockSpec((held, near_count, leaf, leaf), lambda k: (k, 0, 0, 0)),
            pl.BlockSpec((rows, cols), lambda k: (0, 0)),
            pl.BlockSpec((edge, cols), lambda k: (0, 0)),
            pl.BlockSpec((edge, cols), lambda k: (0, 0)),
        ],
        out_specs=pl.BlockSpec((held * leaf, cols), lambda k: (k, 0)),
        scratch_shapes=[pltpu.VMEM((rows + 2 * edge, cols), BF16)],
        compiler_params=params(60),
        cost_estimate=cost(2 * clusters * near_count * leaf * leaf * cols, 28 << 20),
        name="near",
    )
    near = near(near_blocks, panel, low, high)

    place = lax.axis_index(COL).astype(I32).reshape(1)
    steps = 4
    return pl.pallas_call(
        functools.partial(final_kernel, rank, leaf),
        out_shape=jax.ShapeDtypeStruct((rows, cols), BF16),
        grid_spec=pltpu.PrefetchScalarGridSpec(
            num_scalar_prefetch=1,
            grid=(steps,),
            in_specs=[
                pl.BlockSpec((col_peers // 2, clusters * rank // steps, cols), lambda k, at: (0, k, 0)),
                pl.BlockSpec((rank, rows // steps), lambda k, at: (0, at[0] * steps + k)),
                pl.BlockSpec((rows // steps, cols), lambda k, at: (k, 0)),
            ],
            out_specs=pl.BlockSpec((rows // steps, cols), lambda k, at: (k, 0)),
        ),
        compiler_params=params(32),
        cost_estimate=cost(4 * rows * rank * cols, 8 << 20),
        name="final",
    )(place, parts, row_basis.T, near)


def solution(mesh):
    devices = mesh.devices.reshape(2, 4, 4, 2, 2)
    fine = Mesh(devices, ("zl", "y", "x", "zh", "core"))
    placed = (
        P((*ROW, *COL), None),
        P(ROW, None),
        P((*ROW, *COL), None),
        P((*ROW, *COL), None, None, None),
        P(ROW, COL, None, None, None),
        P(ROW, COL, None),
        P(ROW, COL, None),
        P(ROW, COL),
    )
    return jax.shard_map(on_device, mesh=fine, in_specs=placed, out_specs=P((*ROW, *COL), None), check_vma=False)
```

```python
import functools

import jax
import jax.numpy as jnp
from jax import lax
from jax.experimental import pallas as pl
from jax.experimental.pallas import tpu as pltpu
from jax.sharding import Mesh, PartitionSpec as P


F32, BF16, I32 = jnp.float32, jnp.bfloat16, jnp.int32
ROW, COL = ("zl", "y"), ("x", "zh", "core")
NT = (((1,), (1,)), ((), ()))
TN = (((0,), (0,)), ((), ()))
VMEM = pl.BlockSpec(memory_space=pltpu.VMEM)
SMEM = pl.BlockSpec(memory_space=pltpu.SMEM)
HBM = pl.BlockSpec(memory_space=pltpu.HBM)


def cost(flops, nbytes):
    return pl.CostEstimate(flops=flops, bytes_accessed=nbytes, transcendentals=0)


def params(mib):
    return pltpu.CompilerParams(vmem_limit_bytes=mib << 20)


def coeff_kernel(
    leaf, rank, chunks, core_ref, panel_ref, vt_ref, own_ref, chip_ref, far_ref, panel, vt, in_sem, v_sem, edge_sem
):
    rows = panel.shape[0]
    size, edge = rows // chunks, chip_ref.shape[0]
    load_v = pltpu.make_async_copy(vt_ref, vt, v_sem)
    load_v.start()
    loads = []
    for c in range(chunks):
        span = pl.ds(c * size, size)
        loads.append(pltpu.make_async_copy(panel_ref.at[span], panel.at[span], in_sem.at[c]))
        loads[-1].start()
    load_v.wait()
    for c in range(chunks):
        loads[c].wait()
        for k in range(c * size // leaf, (c + 1) * size // leaf):
            span = pl.ds(k * leaf, leaf)
            own_ref[pl.ds(k * rank, rank), :] = jnp.dot(
                vt[:, span], panel[span, :], preferred_element_type=F32
            ).astype(BF16)
    tail = jnp.where(core_ref[0] == 0, rows - edge, 0)
    head = rows - edge - tail
    stores = [
        pltpu.make_async_copy(panel.at[pl.ds(pl.multiple_of(at, edge), edge)], ref, edge_sem.at[i])
        for i, (at, ref) in enumerate(((tail, chip_ref), (head, far_ref)))
    ]
    for store in stores:
        store.start()
    for store in stores:
        store.wait()


def prep_kernel(per_dev, rank, groups, info_ref, rows_ref, cols_ref, x_ref, ct_ref, table_ref):
    slots = rows_ref.shape[1]
    count, core = info_ref[0], info_ref[1]
    lane = lax.broadcasted_iota(I32, (1, slots), 1)
    live = lane < count
    rows = rows_ref[...]
    dest, local = rows // per_dev, rows % per_dev
    other = jnp.where(dest % 2 == core, 1, 0)
    row_key = other * (groups // 2) + (dest // 2) * per_dev + local
    key = jnp.where(live, row_key, groups) * slots + lane
    down = lax.broadcasted_iota(I32, (slots, slots), 0)
    across = lax.broadcasted_iota(I32, (slots, slots), 1)
    key_down = jnp.sum(jnp.where(down == across, key, 0), axis=1, keepdims=True)
    place = jnp.sum((key_down < key).astype(I32), axis=0, keepdims=True)
    place = jnp.where(live, place, -1)
    pick = (down == place).astype(F32).astype(BF16)
    value = lax.dot_general(pick, x_ref[...], NT, preferred_element_type=F32)
    width = value.shape[1]
    k_of = lax.broadcasted_iota(I32, value.shape, 0)
    i_of = lax.broadcasted_iota(I32, value.shape, 1) // rank
    step = 1
    while step < rank:
        k_bit, i_bit = (k_of // step) % 2, (i_of // step) % 2
        ahead = pltpu.roll(pltpu.roll(value, slots - step, 0), step * rank, 1)
        behind = pltpu.roll(pltpu.roll(value, step, 0), width - step * rank, 1)
        value = jnp.where(k_bit == i_bit, value, jnp.where(k_bit == 0, ahead, behind))
        step *= 2
    ct_ref[...] = value.astype(BF16)
    top = jnp.max(jnp.where(live, row_key, 0))
    cols = cols_ref[...] ^ (info_ref[2] * per_dev)
    pair = jnp.concatenate([cols, row_key] + [jnp.zeros_like(row_key)] * 6, axis=0)
    table = lax.dot_general(pair.astype(F32).astype(BF16), pick, NT, preferred_element_type=F32).astype(I32)
    which = lax.broadcasted_iota(I32, table.shape, 0)
    past = lax.broadcasted_iota(I32, table.shape, 1) >= count
    table_ref[...] = jnp.where(past & (which == 1), top, table)


def block_kernel(rank, tile, unroll, table_ref, ct_ref, *refs):
    *parts, own_ref, other_ref, out_ref, g_ref = refs
    slots = table_ref.shape[1]
    cols = g_ref.shape[1]
    size = parts[0].shape[0]
    for j, part in enumerate(parts):
        g_ref[pl.ds(j * size, size), :] = part[...]
    out_ref[...] = jnp.zeros_like(out_ref)
    width = tile * rank
    group = lax.broadcasted_iota(I32, (rank, width), 1) // rank
    masks = [(group == k).astype(F32).astype(BF16) for k in range(tile)]
    halves = ct_ref.shape[1] // width

    def body(step, carry):
        acc, last = carry
        for u in range(unroll):
            for h in range(halves):
                base = (step * unroll + u) * tile * halves + h * tile
                ct = ct_ref[pl.ds(pl.multiple_of((step * unroll + u) * rank, rank), rank), h * width : (h + 1) * width]
                lhs = jnp.concatenate([ct * m for m in masks], axis=0)
                rhs = jnp.concatenate(
                    [
                        g_ref[pl.ds(pl.multiple_of(table_ref[0, base + k] * rank, rank), rank), :]
                        for k in range(tile)
                    ],
                    axis=0,
                )
                terms = jnp.dot(lhs, rhs, preferred_element_type=F32)
                for k in range(tile):
                    row = table_ref[1, base + k]
                    term = terms[k * rank : (k + 1) * rank, :]
                    acc = term + jnp.where(row == last, acc, 0.0)
                    last = row
                    out_ref[pl.ds(pl.multiple_of(row * rank, rank), rank), :] = acc.astype(BF16)
        return acc, last

    steps = slots // (tile * halves * unroll)
    lax.fori_loop(0, steps, body, (jnp.zeros((rank, cols), F32), jnp.int32(-1)))
    size = own_ref.shape[0]
    other_ref[...] = out_ref[pl.ds(0, size), :]
    own_ref[...] = out_ref[pl.ds(size, size), :]


def pair_kernel(chunks, a_ref, b_ref, out_ref, out, sem):
    size = out.shape[0] // chunks
    stores = []
    for c in range(chunks):
        span = pl.ds(c * size, size)
        out[span, :] = (a_ref[span, :].astype(F32) + b_ref[span, :].astype(F32)).astype(BF16)
        stores.append(pltpu.make_async_copy(out.at[span], out_ref.at[span], sem.at[c]))
        stores[-1].start()
    for store in stores:
        store.wait()


def near_kernel(
    group, core_ref, nb_ref, panel_ref, chip_ref, far_ref, out_ref, window, blocks, out, w_sem, nb_sem, out_sem
):
    clusters, near_count, leaf, _ = nb_ref.shape
    rows, edge = panel_ref.shape[0], chip_ref.shape[0]

    def load(k):
        return pltpu.make_async_copy(nb_ref.at[k], blocks.at[k], nb_sem.at[k])

    def store(p):
        span = pl.ds(pl.multiple_of(p * group * leaf, leaf), group * leaf)
        return pltpu.make_async_copy(out.at[span], out_ref.at[span], out_sem.at[p])

    chip_at = jnp.where(core_ref[0] == 0, edge + rows, 0)
    far_at = edge + rows - chip_at
    fills = [
        pltpu.make_async_copy(ref, window.at[pl.ds(pl.multiple_of(at, leaf), ref.shape[0])], w_sem.at[i])
        for i, (at, ref) in enumerate(((edge, panel_ref), (chip_at, chip_ref), (far_at, far_ref)))
    ]
    for fill in fills:
        fill.start()
    for k in range(clusters):
        load(k).start()
    for fill in fills:
        fill.wait()

    def body(p, carry):
        for c in range(group):
            load(p * group + c).wait()
        for c in range(group):
            k = p * group + c
            lhs = jnp.concatenate([blocks[k, o] for o in range(near_count)], axis=1)
            rhs = window[pl.ds(pl.multiple_of(k * leaf, leaf), near_count * leaf), :]
            out[pl.ds(pl.multiple_of(k * leaf, leaf), leaf), :] = jnp.dot(
                lhs, rhs, preferred_element_type=F32
            ).astype(BF16)
        store(p).start()
        return carry

    lax.fori_loop(0, clusters // group, body, 0)
    for p in range(clusters // group):
        store(p).wait()


def final_kernel(
    rank, leaf, place_ref, parts, ut_ref, near_ref, out_ref,
    ut, near, out, ut_sem, near_sem, out_sem,
):
    rows = out.shape[0]
    chunks = near_sem.shape[0]
    size = rows // chunks
    loads = [pltpu.make_async_copy(ut_ref.at[:, pl.ds(pl.multiple_of(place_ref[0] * rows, rows), rows)], ut, ut_sem)]
    for c in range(chunks):
        span = pl.ds(c * size, size)
        loads.append(pltpu.make_async_copy(near_ref.at[span], near.at[span], near_sem.at[c]))
    for load in loads:
        load.start()
    loads[0].wait()
    stores = []
    for c in range(chunks):
        loads[1 + c].wait()
        for k in range(c * size // leaf, (c + 1) * size // leaf):
            span, ranks = pl.ds(k * leaf, leaf), pl.ds(k * rank, rank)
            coupled = parts[0, ranks, :].astype(F32)
            for p in range(1, parts.shape[0]):
                coupled = coupled + parts[p, ranks, :].astype(F32)
            high = coupled.astype(BF16)
            low = (coupled - high.astype(F32)).astype(BF16)
            both = jnp.concatenate([ut[:, span]] * 2, axis=0)
            far = lax.dot_general(both, jnp.concatenate([high, low], axis=0), TN, preferred_element_type=F32)
            out[span, :] = (near[span, :].astype(F32) + far).astype(BF16)
        span = pl.ds(c * size, size)
        stores.append(pltpu.make_async_copy(out.at[span], out_ref.at[span], out_sem.at[c]))
        stores[-1].start()
    for store in stores:
        store.wait()


def on_device(panel, row_basis, col_basis, near_blocks, couplings, blk_rows, blk_cols, blk_count):
    rows, cols = panel.shape
    clusters, near_count, leaf, _ = near_blocks.shape
    rank, slots = col_basis.shape[1], couplings.shape[2]
    half = near_count // 2
    row_peers, col_peers = lax.axis_size(ROW), lax.axis_size(COL)
    groups = col_peers * clusters
    core = lax.axis_index("core")

    edge = half * leaf
    chunks = 4
    here = core.astype(I32).reshape(1)
    coeffs = pl.pallas_call(
        functools.partial(coeff_kernel, leaf, rank, chunks),
        out_shape=(
            jax.ShapeDtypeStruct((clusters * rank, cols), BF16),
            jax.ShapeDtypeStruct((edge, cols), BF16),
            jax.ShapeDtypeStruct((edge, cols), BF16),
        ),
        in_specs=[SMEM, HBM, HBM],
        out_specs=(VMEM, HBM, HBM),
        scratch_shapes=[
            pltpu.VMEM((rows, cols), BF16),
            pltpu.VMEM((rank, rows), BF16),
            pltpu.SemaphoreType.DMA((chunks,)),
            pltpu.SemaphoreType.DMA,
            pltpu.SemaphoreType.DMA((2,)),
        ],
        compiler_params=params(52),
        cost_estimate=cost(2 * rows * rank * cols, 5 << 20),
        name="coeffs",
    )
    own, to_chip, to_far = coeffs(here, panel, col_basis.T)

    def swap_over(x, axis, bits):
        n = lax.axis_size(axis)
        return lax.ppermute(x, axis, [(i, i ^ bits) for i in range(n)])

    y_peers = lax.axis_size("y")
    order = (1, 3, 2)
    across = swap_over(own, "zl", 1)
    held_rows = {0: own, y_peers: across}
    for bits in order:
        held_rows[bits] = swap_over(own, "y", bits)
    for bits in order:
        held_rows[y_peers + bits] = swap_over(across, "y", bits)
    gathered = [held_rows[j] for j in range(row_peers)]

    every = ROW + COL
    peers = lax.axis_size(every)
    from_chip = swap_over(to_chip, "core", 1)
    pairs = [(i, i + 1) for i in range(1, peers - 1, 2)]
    from_far = lax.ppermute(to_far, every, pairs + [(b, a) for a, b in pairs])

    info = jnp.stack([blk_count.reshape(()), core.astype(I32), lax.axis_index(ROW).astype(I32)])
    x = jnp.transpose(couplings.reshape(slots, rank, rank), (1, 2, 0)).reshape(rank * rank, slots)
    prep = pl.pallas_call(
        functools.partial(prep_kernel, clusters, rank, groups),
        out_shape=(jax.ShapeDtypeStruct((slots, rank * rank), BF16), jax.ShapeDtypeStruct((8, slots), I32)),
        in_specs=[SMEM, VMEM, VMEM, VMEM],
        out_specs=(VMEM, VMEM),
        compiler_params=params(24),
        cost_estimate=cost(2 * slots * slots * rank * rank, 1 << 20),
        name="prep",
    )
    ct, table = prep(info, blk_rows.reshape(1, slots), blk_cols.reshape(1, slots), x)

    half_rows = groups // 2 * rank

    blocks = pl.pallas_call(
        functools.partial(block_kernel, rank, 128 // rank, 4),
        out_shape=[jax.ShapeDtypeStruct((half_rows, cols), BF16)] * 2,
        in_specs=[SMEM] + [VMEM] * (1 + row_peers),
        out_specs=[VMEM, VMEM],
        scratch_shapes=[
            pltpu.VMEM((groups * rank, cols), BF16),
            pltpu.VMEM((row_peers * clusters * rank, cols), BF16),
        ],
        compiler_params=params(24),
        cost_estimate=cost(2 * slots * rank * 128 * cols, 4 << 20),
        name="blocks",
    )
    mine, theirs = blocks(table, ct, *gathered)
    swapped = swap_over(theirs, "core", 1)
    summed = pl.pallas_call(
        functools.partial(pair_kernel, chunks),
        out_shape=jax.ShapeDtypeStruct(mine.shape, BF16),
        in_specs=[VMEM, VMEM],
        out_specs=HBM,
        scratch_shapes=[pltpu.VMEM(mine.shape, BF16), pltpu.SemaphoreType.DMA((chunks,))],
        compiler_params=params(44),
        cost_estimate=cost(mine.size, 3 << 20),
        name="pair",
    )(mine, swapped)
    parts = lax.all_to_all(
        summed.reshape(col_peers // 2, clusters * rank, cols), ("x", "zh"), 0, 0, tiled=True
    )

    group = 2
    near_call = pl.pallas_call(
        functools.partial(near_kernel, group),
        out_shape=jax.ShapeDtypeStruct((rows, cols), BF16),
        in_specs=[SMEM, HBM, HBM, HBM, HBM],
        out_specs=HBM,
        scratch_shapes=[
            pltpu.VMEM((rows + 2 * edge, cols), BF16),
            pltpu.VMEM(near_blocks.shape, BF16),
            pltpu.VMEM((rows, cols), BF16),
            pltpu.SemaphoreType.DMA((3,)),
            pltpu.SemaphoreType.DMA((clusters,)),
            pltpu.SemaphoreType.DMA((clusters // group,)),
        ],
        compiler_params=params(52),
        cost_estimate=cost(2 * clusters * near_count * leaf * leaf * cols, 24 << 20),
        name="near",
    )
    near = near_call(here, near_blocks, panel, from_chip, from_far)

    place = lax.axis_index(COL).astype(I32).reshape(1)
    return pl.pallas_call(
        functools.partial(final_kernel, rank, leaf),
        out_shape=jax.ShapeDtypeStruct((rows, cols), BF16),
        in_specs=[SMEM, VMEM, HBM, HBM],
        out_specs=HBM,
        scratch_shapes=[
            pltpu.VMEM((rank, rows), BF16),
            pltpu.VMEM((rows, cols), BF16),
            pltpu.VMEM((rows, cols), BF16),
            pltpu.SemaphoreType.DMA,
            pltpu.SemaphoreType.DMA((chunks,)),
            pltpu.SemaphoreType.DMA((chunks,)),
        ],
        compiler_params=params(52),
        cost_estimate=cost(4 * rows * rank * cols, 8 << 20),
        name="final",
    )(place, parts, row_basis.T, near)


def solution(mesh):
    devices = mesh.devices.reshape(2, 4, 4, 2, 2)
    fine = Mesh(devices, ("zl", "y", "x", "zh", "core"))
    placed = (
        P((*ROW, *COL), None),
        P(ROW, None),
        P((*ROW, *COL), None),
        P((*ROW, *COL), None, None, None),
        P(ROW, COL, None, None, None),
        P(ROW, COL, None),
        P(ROW, COL, None),
        P(ROW, COL),
    )
    return jax.shard_map(on_device, mesh=fine, in_specs=placed, out_specs=P((*ROW, *COL), None), check_vma=False)
```

```python
import functools

import jax
import jax.numpy as jnp
from jax import lax
from jax.experimental import pallas as pl
from jax.experimental.pallas import tpu as pltpu
from jax.sharding import Mesh, PartitionSpec as P


F32, BF16, I32 = jnp.float32, jnp.bfloat16, jnp.int32
ROW, COL = ("zl", "y"), ("x", "zh", "core")
NT = (((1,), (1,)), ((), ()))
TN = (((0,), (0,)), ((), ()))
VMEM = pl.BlockSpec(memory_space=pltpu.VMEM)
SMEM = pl.BlockSpec(memory_space=pltpu.SMEM)
HBM = pl.BlockSpec(memory_space=pltpu.HBM)


def cost(flops, nbytes):
    return pl.CostEstimate(flops=flops, bytes_accessed=nbytes, transcendentals=0)


def params(mib):
    return pltpu.CompilerParams(vmem_limit_bytes=mib << 20)


def coeff_kernel(
    leaf, rank, chunks, core_ref, panel_ref, vt_ref, own_ref, chip_ref, far_ref, panel, vt, in_sem, v_sem, edge_sem
):
    rows = panel.shape[0]
    size, edge = rows // chunks, chip_ref.shape[0]
    load_v = pltpu.make_async_copy(vt_ref, vt, v_sem)
    load_v.start()
    loads = []
    for c in range(chunks):
        span = pl.ds(c * size, size)
        loads.append(pltpu.make_async_copy(panel_ref.at[span], panel.at[span], in_sem.at[c]))
        loads[-1].start()
    load_v.wait()
    for c in range(chunks):
        loads[c].wait()
        for k in range(c * size // leaf, (c + 1) * size // leaf):
            span = pl.ds(k * leaf, leaf)
            own_ref[pl.ds(k * rank, rank), :] = jnp.dot(
                vt[:, span], panel[span, :], preferred_element_type=F32
            ).astype(BF16)
    tail = jnp.where(core_ref[0] == 0, rows - edge, 0)
    head = rows - edge - tail
    stores = [
        pltpu.make_async_copy(panel.at[pl.ds(pl.multiple_of(at, edge), edge)], ref, edge_sem.at[i])
        for i, (at, ref) in enumerate(((tail, chip_ref), (head, far_ref)))
    ]
    for store in stores:
        store.start()
    for store in stores:
        store.wait()


def prep_kernel(per_dev, rank, groups, info_ref, rows_ref, cols_ref, x_ref, ct_ref, table_ref):
    slots = rows_ref.shape[1]
    count, core = info_ref[0], info_ref[1]
    lane = lax.broadcasted_iota(I32, (1, slots), 1)
    live = lane < count
    rows = rows_ref[...]
    dest, local = rows // per_dev, rows % per_dev
    other = jnp.where(dest % 2 == core, 1, 0)
    row_key = other * (groups // 2) + (dest // 2) * per_dev + local
    key = jnp.where(live, row_key, groups) * slots + lane
    down = lax.broadcasted_iota(I32, (slots, slots), 0)
    across = lax.broadcasted_iota(I32, (slots, slots), 1)
    key_down = jnp.sum(jnp.where(down == across, key, 0), axis=1, keepdims=True)
    place = jnp.sum((key_down < key).astype(I32), axis=0, keepdims=True)
    place = jnp.where(live, place, -1)
    pick = (down == place).astype(F32).astype(BF16)
    value = lax.dot_general(pick, x_ref[...], NT, preferred_element_type=F32)
    width = value.shape[1]
    k_of = lax.broadcasted_iota(I32, value.shape, 0)
    i_of = lax.broadcasted_iota(I32, value.shape, 1) // rank
    step = 1
    while step < rank:
        k_bit, i_bit = (k_of // step) % 2, (i_of // step) % 2
        ahead = pltpu.roll(pltpu.roll(value, slots - step, 0), step * rank, 1)
        behind = pltpu.roll(pltpu.roll(value, step, 0), width - step * rank, 1)
        value = jnp.where(k_bit == i_bit, value, jnp.where(k_bit == 0, ahead, behind))
        step *= 2
    ct_ref[...] = value.astype(BF16)
    top = jnp.max(jnp.where(live, row_key, 0))
    ahead = jnp.sum((live & (row_key < groups // 2)).astype(I32))
    cols = cols_ref[...] ^ (info_ref[2] * per_dev)
    pair = jnp.concatenate([cols, row_key] + [jnp.zeros_like(row_key)] * 6, axis=0)
    table = lax.dot_general(pair.astype(F32).astype(BF16), pick, NT, preferred_element_type=F32).astype(I32)
    which = lax.broadcasted_iota(I32, table.shape, 0)
    past = lax.broadcasted_iota(I32, table.shape, 1) >= count
    table = jnp.where(past & (which == 1), top, table)
    table_ref[...] = jnp.where(which == 2, ahead, jnp.where(which == 3, count, table))


def block_kernel(rank, tile, unroll, second, table_ref, ct_ref, *refs):
    *parts, out_ref = refs
    if second:
        (g_ref,) = parts
    else:
        *parts, out_ref, g_ref = refs
        size = parts[0].shape[0]
        for j, part in enumerate(parts):
            g_ref[pl.ds(j * size, size), :] = part[...]
    cols = g_ref.shape[1]
    held = out_ref.shape[0] // rank - 1
    out_ref[...] = jnp.zeros_like(out_ref)
    width = tile * rank
    group = lax.broadcasted_iota(I32, (rank, width), 1) // rank
    masks = [(group == k).astype(F32).astype(BF16) for k in range(tile)]
    halves = ct_ref.shape[1] // width
    per_step = tile * halves * unroll

    def body(step, carry):
        acc, last = carry
        for u in range(unroll):
            at = pl.multiple_of((step * unroll + u) * rank, rank)
            for h in range(halves):
                base = step * per_step + (u * halves + h) * tile
                ct = ct_ref[pl.ds(at, rank), h * width : (h + 1) * width]
                lhs = jnp.concatenate([ct * m for m in masks], axis=0)
                rhs = jnp.concatenate(
                    [
                        g_ref[pl.ds(pl.multiple_of(table_ref[0, base + k] * rank, rank), rank), :]
                        for k in range(tile)
                    ],
                    axis=0,
                )
                terms = jnp.dot(lhs, rhs, preferred_element_type=F32)
                for k in range(tile):
                    row = table_ref[1, base + k]
                    term = terms[k * rank : (k + 1) * rank, :]
                    acc = term + jnp.where(row == last, acc, 0.0)
                    last = row
                    spot = row - held if second else row
                    inside = spot >= 0 if second else spot < held
                    spot = jnp.where(inside, spot, held)
                    out_ref[pl.ds(pl.multiple_of(spot * rank, rank), rank), :] = acc.astype(BF16)
        return acc, last

    ahead, count = table_ref[2, 0], table_ref[3, 0]
    first = ahead // per_step if second else 0
    end = ((count if second else ahead) + per_step - 1) // per_step
    lax.fori_loop(first, end, body, (jnp.zeros((rank, cols), F32), jnp.int32(-1)))


def pair_kernel(chunks, a_ref, b_ref, out_ref, out, sem):
    size = out.shape[0] // chunks
    stores = []
    for c in range(chunks):
        span = pl.ds(c * size, size)
        out[span, :] = (a_ref[span, :].astype(F32) + b_ref[span, :].astype(F32)).astype(BF16)
        stores.append(pltpu.make_async_copy(out.at[span], out_ref.at[span], sem.at[c]))
        stores[-1].start()
    for store in stores:
        store.wait()


def near_kernel(
    group, core_ref, nb_ref, panel_ref, chip_ref, far_ref, out_ref, window, blocks, out, w_sem, nb_sem, out_sem
):
    clusters, near_count, leaf, _ = nb_ref.shape
    rows, edge = panel_ref.shape[0], chip_ref.shape[0]

    def load(k):
        return pltpu.make_async_copy(nb_ref.at[k], blocks.at[k], nb_sem.at[k])

    def store(p):
        span = pl.ds(pl.multiple_of(p * group * leaf, leaf), group * leaf)
        return pltpu.make_async_copy(out.at[span], out_ref.at[span], out_sem.at[p])

    chip_at = jnp.where(core_ref[0] == 0, edge + rows, 0)
    far_at = edge + rows - chip_at
    fills = [
        pltpu.make_async_copy(ref, window.at[pl.ds(pl.multiple_of(at, leaf), ref.shape[0])], w_sem.at[i])
        for i, (at, ref) in enumerate(((edge, panel_ref), (chip_at, chip_ref), (far_at, far_ref)))
    ]
    for fill in fills:
        fill.start()
    for k in range(clusters):
        load(k).start()
    for fill in fills:
        fill.wait()

    def body(p, carry):
        for c in range(group):
            load(p * group + c).wait()
        for c in range(group):
            k = p * group + c
            lhs = jnp.concatenate([blocks[k, o] for o in range(near_count)], axis=1)
            rhs = window[pl.ds(pl.multiple_of(k * leaf, leaf), near_count * leaf), :]
            out[pl.ds(pl.multiple_of(k * leaf, leaf), leaf), :] = jnp.dot(
                lhs, rhs, preferred_element_type=F32
            ).astype(BF16)
        store(p).start()
        return carry

    lax.fori_loop(0, clusters // group, body, 0)
    for p in range(clusters // group):
        store(p).wait()


def final_kernel(
    rank, leaf, place_ref, parts, ut_ref, near_ref, out_ref,
    ut, near, out, ut_sem, near_sem, out_sem,
):
    rows = out.shape[0]
    chunks = near_sem.shape[0]
    size = rows // chunks
    loads = [pltpu.make_async_copy(ut_ref.at[:, pl.ds(pl.multiple_of(place_ref[0] * rows, rows), rows)], ut, ut_sem)]
    for c in range(chunks):
        span = pl.ds(c * size, size)
        loads.append(pltpu.make_async_copy(near_ref.at[span], near.at[span], near_sem.at[c]))
    for load in loads:
        load.start()
    loads[0].wait()
    stores = []
    for c in range(chunks):
        loads[1 + c].wait()
        for k in range(c * size // leaf, (c + 1) * size // leaf):
            span, ranks = pl.ds(k * leaf, leaf), pl.ds(k * rank, rank)
            coupled = parts[0, ranks, :].astype(F32)
            for p in range(1, parts.shape[0]):
                coupled = coupled + parts[p, ranks, :].astype(F32)
            high = coupled.astype(BF16)
            low = (coupled - high.astype(F32)).astype(BF16)
            both = jnp.concatenate([ut[:, span]] * 2, axis=0)
            far = lax.dot_general(both, jnp.concatenate([high, low], axis=0), TN, preferred_element_type=F32)
            out[span, :] = (near[span, :].astype(F32) + far).astype(BF16)
        span = pl.ds(c * size, size)
        stores.append(pltpu.make_async_copy(out.at[span], out_ref.at[span], out_sem.at[c]))
        stores[-1].start()
    for store in stores:
        store.wait()


def on_device(panel, row_basis, col_basis, near_blocks, couplings, blk_rows, blk_cols, blk_count):
    rows, cols = panel.shape
    clusters, near_count, leaf, _ = near_blocks.shape
    rank, slots = col_basis.shape[1], couplings.shape[2]
    half = near_count // 2
    row_peers, col_peers = lax.axis_size(ROW), lax.axis_size(COL)
    groups = col_peers * clusters
    core = lax.axis_index("core")

    edge = half * leaf
    chunks = 4
    here = core.astype(I32).reshape(1)
    coeffs = pl.pallas_call(
        functools.partial(coeff_kernel, leaf, rank, chunks),
        out_shape=(
            jax.ShapeDtypeStruct((clusters * rank, cols), BF16),
            jax.ShapeDtypeStruct((edge, cols), BF16),
            jax.ShapeDtypeStruct((edge, cols), BF16),
        ),
        in_specs=[SMEM, HBM, HBM],
        out_specs=(VMEM, HBM, HBM),
        scratch_shapes=[
            pltpu.VMEM((rows, cols), BF16),
            pltpu.VMEM((rank, rows), BF16),
            pltpu.SemaphoreType.DMA((chunks,)),
            pltpu.SemaphoreType.DMA,
            pltpu.SemaphoreType.DMA((2,)),
        ],
        compiler_params=params(52),
        cost_estimate=cost(2 * rows * rank * cols, 5 << 20),
        name="coeffs",
    )
    own, to_chip, to_far = coeffs(here, panel, col_basis.T)

    def swap_over(x, axis, bits):
        n = lax.axis_size(axis)
        return lax.ppermute(x, axis, [(i, i ^ bits) for i in range(n)])

    y_peers = lax.axis_size("y")
    order = (1, 3, 2)
    across = swap_over(own, "zl", 1)
    held_rows = {0: own, y_peers: across}
    for bits in order:
        held_rows[bits] = swap_over(own, "y", bits)
    for bits in order:
        held_rows[y_peers + bits] = swap_over(across, "y", bits)
    gathered = [held_rows[j] for j in range(row_peers)]

    every = ROW + COL
    peers = lax.axis_size(every)
    from_chip = swap_over(to_chip, "core", 1)
    pairs = [(i, i + 1) for i in range(1, peers - 1, 2)]
    from_far = lax.ppermute(to_far, every, pairs + [(b, a) for a, b in pairs])

    info = jnp.stack([blk_count.reshape(()), core.astype(I32), lax.axis_index(ROW).astype(I32)])
    x = jnp.transpose(couplings.reshape(slots, rank, rank), (1, 2, 0)).reshape(rank * rank, slots)
    prep = pl.pallas_call(
        functools.partial(prep_kernel, clusters, rank, groups),
        out_shape=(jax.ShapeDtypeStruct((slots, rank * rank), BF16), jax.ShapeDtypeStruct((8, slots), I32)),
        in_specs=[SMEM, VMEM, VMEM, VMEM],
        out_specs=(VMEM, VMEM),
        compiler_params=params(24),
        cost_estimate=cost(2 * slots * slots * rank * rank, 1 << 20),
        name="prep",
    )
    ct, table = prep(info, blk_rows.reshape(1, slots), blk_cols.reshape(1, slots), x)

    half_rows = groups // 2 * rank

    kept = jax.ShapeDtypeStruct((half_rows + rank, cols), BF16)

    def blocks(second):
        held_shape = jax.ShapeDtypeStruct((row_peers * clusters * rank, cols), BF16)
        return pl.pallas_call(
            functools.partial(block_kernel, rank, 128 // rank, 2, second),
            out_shape=kept if second else (kept, held_shape),
            in_specs=[SMEM] + [VMEM] * (2 if second else 1 + row_peers),
            out_specs=VMEM if second else (VMEM, VMEM),
            compiler_params=params(24),
            cost_estimate=cost(slots * rank * 128 * cols, 2 << 20),
            name="blocks_own" if second else "blocks_other",
        )

    theirs, held_all = blocks(False)(table, ct, *gathered)
    swapped = swap_over(theirs, "core", 1)
    mine = blocks(True)(table, ct, held_all)
    summed = pl.pallas_call(
        functools.partial(pair_kernel, chunks),
        out_shape=jax.ShapeDtypeStruct((half_rows, cols), BF16),
        in_specs=[VMEM, VMEM],
        out_specs=HBM,
        scratch_shapes=[pltpu.VMEM((half_rows, cols), BF16), pltpu.SemaphoreType.DMA((chunks,))],
        compiler_params=params(44),
        cost_estimate=cost(mine.size, 3 << 20),
        name="pair",
    )(mine, swapped)
    parts = lax.all_to_all(
        summed.reshape(col_peers // 2, clusters * rank, cols), ("x", "zh"), 0, 0, tiled=True
    )

    group = 2
    near_call = pl.pallas_call(
        functools.partial(near_kernel, group),
        out_shape=jax.ShapeDtypeStruct((rows, cols), BF16),
        in_specs=[SMEM, HBM, HBM, HBM, HBM],
        out_specs=HBM,
        scratch_shapes=[
            pltpu.VMEM((rows + 2 * edge, cols), BF16),
            pltpu.VMEM(near_blocks.shape, BF16),
            pltpu.VMEM((rows, cols), BF16),
            pltpu.SemaphoreType.DMA((3,)),
            pltpu.SemaphoreType.DMA((clusters,)),
            pltpu.SemaphoreType.DMA((clusters // group,)),
        ],
        compiler_params=params(52),
        cost_estimate=cost(2 * clusters * near_count * leaf * leaf * cols, 24 << 20),
        name="near",
    )
    near = near_call(here, near_blocks, panel, from_chip, from_far)

    place = lax.axis_index(COL).astype(I32).reshape(1)
    return pl.pallas_call(
        functools.partial(final_kernel, rank, leaf),
        out_shape=jax.ShapeDtypeStruct((rows, cols), BF16),
        in_specs=[SMEM, VMEM, HBM, HBM],
        out_specs=HBM,
        scratch_shapes=[
            pltpu.VMEM((rank, rows), BF16),
            pltpu.VMEM((rows, cols), BF16),
            pltpu.VMEM((rows, cols), BF16),
            pltpu.SemaphoreType.DMA,
            pltpu.SemaphoreType.DMA((chunks,)),
            pltpu.SemaphoreType.DMA((chunks,)),
        ],
        compiler_params=params(52),
        cost_estimate=cost(4 * rows * rank * cols, 8 << 20),
        name="final",
    )(place, parts, row_basis.T, near)


def solution(mesh):
    devices = mesh.devices.reshape(2, 4, 4, 2, 2)
    fine = Mesh(devices, ("zl", "y", "x", "zh", "core"))
    placed = (
        P((*ROW, *COL), None),
        P(ROW, None),
        P((*ROW, *COL), None),
        P((*ROW, *COL), None, None, None),
        P(ROW, COL, None, None, None),
        P(ROW, COL, None),
        P(ROW, COL, None),
        P(ROW, COL),
    )
    return jax.shard_map(on_device, mesh=fine, in_specs=placed, out_specs=P((*ROW, *COL), None), check_vma=False)
```

```python
import functools

import jax
import jax.numpy as jnp
from jax import lax
from jax.experimental import pallas as pl
from jax.experimental.pallas import tpu as pltpu
from jax.sharding import Mesh, PartitionSpec as P


F32, BF16, I32 = jnp.float32, jnp.bfloat16, jnp.int32
ROW, COL = ("zl", "y"), ("x", "zh", "core")
NT = (((1,), (1,)), ((), ()))
TN = (((0,), (0,)), ((), ()))
VMEM = pl.BlockSpec(memory_space=pltpu.VMEM)
SMEM = pl.BlockSpec(memory_space=pltpu.SMEM)
HBM = pl.BlockSpec(memory_space=pltpu.HBM)


def cost(flops, nbytes):
    return pl.CostEstimate(flops=flops, bytes_accessed=nbytes, transcendentals=0)


def params(mib):
    return pltpu.CompilerParams(vmem_limit_bytes=mib << 20)


def coeff_kernel(
    leaf, rank, chunks, core_ref, panel_ref, vt_ref, own_ref, chip_ref, far_ref, panel, vt, in_sem, v_sem, edge_sem
):
    rows = panel.shape[0]
    size, edge = rows // chunks, chip_ref.shape[0]
    load_v = pltpu.make_async_copy(vt_ref, vt, v_sem)
    load_v.start()
    loads = []
    for c in range(chunks):
        span = pl.ds(c * size, size)
        loads.append(pltpu.make_async_copy(panel_ref.at[span], panel.at[span], in_sem.at[c]))
        loads[-1].start()
    load_v.wait()
    for c in range(chunks):
        loads[c].wait()
        for k in range(c * size // leaf, (c + 1) * size // leaf):
            span = pl.ds(k * leaf, leaf)
            own_ref[pl.ds(k * rank, rank), :] = jnp.dot(
                vt[:, span], panel[span, :], preferred_element_type=F32
            ).astype(BF16)
    tail = jnp.where(core_ref[0] == 0, rows - edge, 0)
    head = rows - edge - tail
    stores = [
        pltpu.make_async_copy(panel.at[pl.ds(pl.multiple_of(at, edge), edge)], ref, edge_sem.at[i])
        for i, (at, ref) in enumerate(((tail, chip_ref), (head, far_ref)))
    ]
    for store in stores:
        store.start()
    for store in stores:
        store.wait()


def prep_kernel(per_dev, rank, groups, count_ref, core_ref, at_row_ref, rows_ref, cols_ref, x_ref, ct_ref, table_ref):
    slots = rows_ref.shape[1]
    count, core = count_ref[0, 0], core_ref[0]
    lane = lax.broadcasted_iota(I32, (1, slots), 1)
    live = lane < count
    rows = rows_ref[...]
    dest, local = rows // per_dev, rows % per_dev
    other = jnp.where(dest % 2 == core, 1, 0)
    row_key = other * (groups // 2) + (dest // 2) * per_dev + local
    key = jnp.where(live, row_key, groups) * slots + lane
    down = lax.broadcasted_iota(I32, (slots, slots), 0)
    across = lax.broadcasted_iota(I32, (slots, slots), 1)
    key_down = jnp.sum(jnp.where(down == across, key, 0), axis=1, keepdims=True)
    place = jnp.sum((key_down < key).astype(I32), axis=0, keepdims=True)
    place = jnp.where(live, place, -1)
    pick = (down == place).astype(F32).astype(BF16)
    value = lax.dot_general(pick, x_ref[...], NT, preferred_element_type=F32)
    width = value.shape[1]
    k_of = lax.broadcasted_iota(I32, value.shape, 0)
    i_of = lax.broadcasted_iota(I32, value.shape, 1) // rank
    step = 1
    while step < rank:
        k_bit, i_bit = (k_of // step) % 2, (i_of // step) % 2
        ahead = pltpu.roll(pltpu.roll(value, slots - step, 0), step * rank, 1)
        behind = pltpu.roll(pltpu.roll(value, step, 0), width - step * rank, 1)
        value = jnp.where(k_bit == i_bit, value, jnp.where(k_bit == 0, ahead, behind))
        step *= 2
    ct_ref[...] = value.astype(BF16)
    top = jnp.max(jnp.where(live, row_key, 0))
    ahead = jnp.sum((live & (row_key < groups // 2)).astype(I32))
    cols = cols_ref[...] ^ (at_row_ref[0] * per_dev)
    pair = jnp.concatenate([cols, row_key] + [jnp.zeros_like(row_key)] * 6, axis=0)
    table = lax.dot_general(pair.astype(F32).astype(BF16), pick, NT, preferred_element_type=F32).astype(I32)
    which = lax.broadcasted_iota(I32, table.shape, 0)
    past = lax.broadcasted_iota(I32, table.shape, 1) >= count
    table = jnp.where(past & (which == 1), top, table)
    table_ref[...] = jnp.where(which == 2, ahead, jnp.where(which == 3, count, table))


def block_kernel(rank, tile, unroll, second, table_ref, ct_ref, *refs):
    *parts, out_ref = refs
    if second:
        (g_ref,) = parts
    else:
        *parts, out_ref, g_ref = refs
        size = parts[0].shape[0]
        for j, part in enumerate(parts):
            g_ref[pl.ds(j * size, size), :] = part[...]
    cols = g_ref.shape[1]
    held = out_ref.shape[0] // rank - 1
    out_ref[...] = jnp.zeros_like(out_ref)
    width = tile * rank
    group = lax.broadcasted_iota(I32, (rank, width), 1) // rank
    masks = [(group == k).astype(F32).astype(BF16) for k in range(tile)]
    halves = ct_ref.shape[1] // width
    per_step = tile * halves * unroll

    def body(step, carry):
        acc, last = carry
        for u in range(unroll):
            at = pl.multiple_of((step * unroll + u) * rank, rank)
            for h in range(halves):
                base = step * per_step + (u * halves + h) * tile
                ct = ct_ref[pl.ds(at, rank), h * width : (h + 1) * width]
                lhs = jnp.concatenate([ct * m for m in masks], axis=0)
                rhs = jnp.concatenate(
                    [
                        g_ref[pl.ds(pl.multiple_of(table_ref[0, base + k] * rank, rank), rank), :]
                        for k in range(tile)
                    ],
                    axis=0,
                )
                terms = jnp.dot(lhs, rhs, preferred_element_type=F32)
                for k in range(tile):
                    row = table_ref[1, base + k]
                    term = terms[k * rank : (k + 1) * rank, :]
                    acc = term + jnp.where(row == last, acc, 0.0)
                    last = row
                    spot = row - held if second else row
                    inside = spot >= 0 if second else spot < held
                    spot = jnp.where(inside, spot, held)
                    out_ref[pl.ds(pl.multiple_of(spot * rank, rank), rank), :] = acc.astype(BF16)
        return acc, last

    ahead, count = table_ref[2, 0], table_ref[3, 0]
    first = ahead // per_step if second else 0
    end = ((count if second else ahead) + per_step - 1) // per_step
    lax.fori_loop(first, end, body, (jnp.zeros((rank, cols), F32), jnp.int32(-1)))


def pair_kernel(chunks, a_ref, b_ref, out_ref, out, sem):
    size = out.shape[0] // chunks
    stores = []
    for c in range(chunks):
        span = pl.ds(c * size, size)
        out[span, :] = (a_ref[span, :].astype(F32) + b_ref[span, :].astype(F32)).astype(BF16)
        stores.append(pltpu.make_async_copy(out.at[span], out_ref.at[span], sem.at[c]))
        stores[-1].start()
    for store in stores:
        store.wait()


def near_kernel(
    group, core_ref, nb_ref, panel_ref, chip_ref, far_ref, out_ref, window, blocks, out, w_sem, nb_sem, out_sem
):
    clusters, near_count, leaf, _ = nb_ref.shape
    rows, edge = panel_ref.shape[0], chip_ref.shape[0]

    def load(k):
        return pltpu.make_async_copy(nb_ref.at[k], blocks.at[k], nb_sem.at[k])

    def store(p):
        span = pl.ds(pl.multiple_of(p * group * leaf, leaf), group * leaf)
        return pltpu.make_async_copy(out.at[span], out_ref.at[span], out_sem.at[p])

    chip_at = jnp.where(core_ref[0] == 0, edge + rows, 0)
    far_at = edge + rows - chip_at
    fills = [
        pltpu.make_async_copy(ref, window.at[pl.ds(pl.multiple_of(at, leaf), ref.shape[0])], w_sem.at[i])
        for i, (at, ref) in enumerate(((edge, panel_ref), (chip_at, chip_ref), (far_at, far_ref)))
    ]
    for fill in fills:
        fill.start()
    for k in range(clusters):
        load(k).start()
    for fill in fills:
        fill.wait()

    def body(p, carry):
        for c in range(group):
            load(p * group + c).wait()
        for c in range(group):
            k = p * group + c
            lhs = jnp.concatenate([blocks[k, o] for o in range(near_count)], axis=1)
            rhs = window[pl.ds(pl.multiple_of(k * leaf, leaf), near_count * leaf), :]
            out[pl.ds(pl.multiple_of(k * leaf, leaf), leaf), :] = jnp.dot(
                lhs, rhs, preferred_element_type=F32
            ).astype(BF16)
        store(p).start()
        return carry

    lax.fori_loop(0, clusters // group, body, 0)
    for p in range(clusters // group):
        store(p).wait()


def final_kernel(
    rank, leaf, place_ref, parts, ut_ref, near_ref, out_ref,
    ut, near, out, ut_sem, near_sem, out_sem,
):
    rows = out.shape[0]
    chunks = near_sem.shape[0]
    size = rows // chunks
    loads = [pltpu.make_async_copy(ut_ref.at[:, pl.ds(pl.multiple_of(place_ref[0] * rows, rows), rows)], ut, ut_sem)]
    for c in range(chunks):
        span = pl.ds(c * size, size)
        loads.append(pltpu.make_async_copy(near_ref.at[span], near.at[span], near_sem.at[c]))
    for load in loads:
        load.start()
    loads[0].wait()
    stores = []
    for c in range(chunks):
        loads[1 + c].wait()
        for k in range(c * size // leaf, (c + 1) * size // leaf):
            span, ranks = pl.ds(k * leaf, leaf), pl.ds(k * rank, rank)
            coupled = parts[0, ranks, :].astype(F32)
            for p in range(1, parts.shape[0]):
                coupled = coupled + parts[p, ranks, :].astype(F32)
            high = coupled.astype(BF16)
            low = (coupled - high.astype(F32)).astype(BF16)
            both = jnp.concatenate([ut[:, span]] * 2, axis=0)
            far = lax.dot_general(both, jnp.concatenate([high, low], axis=0), TN, preferred_element_type=F32)
            out[span, :] = (near[span, :].astype(F32) + far).astype(BF16)
        span = pl.ds(c * size, size)
        stores.append(pltpu.make_async_copy(out.at[span], out_ref.at[span], out_sem.at[c]))
        stores[-1].start()
    for store in stores:
        store.wait()


def on_device(panel, row_basis, col_basis, near_blocks, couplings, blk_rows, blk_cols, blk_count):
    rows, cols = panel.shape
    clusters, near_count, leaf, _ = near_blocks.shape
    rank, slots = col_basis.shape[1], couplings.shape[2]
    half = near_count // 2
    row_peers, col_peers = lax.axis_size(ROW), lax.axis_size(COL)
    groups = col_peers * clusters
    core = lax.axis_index("core")

    edge = half * leaf
    chunks = 4
    here = core.astype(I32).reshape(1)
    coeffs = pl.pallas_call(
        functools.partial(coeff_kernel, leaf, rank, chunks),
        out_shape=(
            jax.ShapeDtypeStruct((clusters * rank, cols), BF16),
            jax.ShapeDtypeStruct((edge, cols), BF16),
            jax.ShapeDtypeStruct((edge, cols), BF16),
        ),
        in_specs=[SMEM, HBM, HBM],
        out_specs=(VMEM, HBM, HBM),
        scratch_shapes=[
            pltpu.VMEM((rows, cols), BF16),
            pltpu.VMEM((rank, rows), BF16),
            pltpu.SemaphoreType.DMA((chunks,)),
            pltpu.SemaphoreType.DMA,
            pltpu.SemaphoreType.DMA((2,)),
        ],
        compiler_params=params(52),
        cost_estimate=cost(2 * rows * rank * cols, 5 << 20),
        name="coeffs",
    )
    own, to_chip, to_far = coeffs(here, panel, col_basis.T)

    def swap_over(x, axis, bits):
        n = lax.axis_size(axis)
        return lax.ppermute(x, axis, [(i, i ^ bits) for i in range(n)])

    y_peers = lax.axis_size("y")
    order = (1, 3, 2)
    across = swap_over(own, "zl", 1)
    held_rows = {0: own, y_peers: across}
    for bits in order:
        held_rows[bits] = swap_over(own, "y", bits)
    for bits in order:
        held_rows[y_peers + bits] = swap_over(across, "y", bits)
    gathered = [held_rows[j] for j in range(row_peers)]

    every = ROW + COL
    peers = lax.axis_size(every)
    from_chip = swap_over(to_chip, "core", 1)
    pairs = [(i, i + 1) for i in range(1, peers - 1, 2)]
    from_far = lax.ppermute(to_far, every, pairs + [(b, a) for a, b in pairs])

    at_row = lax.axis_index(ROW).astype(I32).reshape(1)
    x = jnp.transpose(couplings.reshape(slots, rank, rank), (1, 2, 0)).reshape(rank * rank, slots)
    prep = pl.pallas_call(
        functools.partial(prep_kernel, clusters, rank, groups),
        out_shape=(jax.ShapeDtypeStruct((slots, rank * rank), BF16), jax.ShapeDtypeStruct((8, slots), I32)),
        in_specs=[SMEM, SMEM, SMEM, VMEM, VMEM, VMEM],
        out_specs=(VMEM, VMEM),
        compiler_params=params(24),
        cost_estimate=cost(2 * slots * slots * rank * rank, 1 << 20),
        name="prep",
    )
    ct, table = prep(blk_count, here, at_row, blk_rows.reshape(1, slots), blk_cols.reshape(1, slots), x)

    half_rows = groups // 2 * rank

    kept = jax.ShapeDtypeStruct((half_rows + rank, cols), BF16)

    def blocks(second):
        held_shape = jax.ShapeDtypeStruct((row_peers * clusters * rank, cols), BF16)
        return pl.pallas_call(
            functools.partial(block_kernel, rank, 128 // rank, 4, second),
            out_shape=kept if second else (kept, held_shape),
            in_specs=[SMEM] + [VMEM] * (2 if second else 1 + row_peers),
            out_specs=VMEM if second else (VMEM, VMEM),
            compiler_params=params(24),
            cost_estimate=cost(slots * rank * 128 * cols, 2 << 20),
            name="blocks_own" if second else "blocks_other",
        )

    theirs, held_all = blocks(False)(table, ct, *gathered)
    swapped = swap_over(theirs, "core", 1)
    mine = blocks(True)(table, ct, held_all)
    summed = pl.pallas_call(
        functools.partial(pair_kernel, chunks),
        out_shape=jax.ShapeDtypeStruct((half_rows, cols), BF16),
        in_specs=[VMEM, VMEM],
        out_specs=HBM,
        scratch_shapes=[pltpu.VMEM((half_rows, cols), BF16), pltpu.SemaphoreType.DMA((chunks,))],
        compiler_params=params(44),
        cost_estimate=cost(mine.size, 3 << 20),
        name="pair",
    )(mine, swapped)
    parts = lax.all_to_all(
        summed.reshape(col_peers // 2, clusters * rank, cols), ("x", "zh"), 0, 0, tiled=True
    )

    group = 2
    near_call = pl.pallas_call(
        functools.partial(near_kernel, group),
        out_shape=jax.ShapeDtypeStruct((rows, cols), BF16),
        in_specs=[SMEM, HBM, HBM, HBM, HBM],
        out_specs=HBM,
        scratch_shapes=[
            pltpu.VMEM((rows + 2 * edge, cols), BF16),
            pltpu.VMEM(near_blocks.shape, BF16),
            pltpu.VMEM((rows, cols), BF16),
            pltpu.SemaphoreType.DMA((3,)),
            pltpu.SemaphoreType.DMA((clusters,)),
            pltpu.SemaphoreType.DMA((clusters // group,)),
        ],
        compiler_params=params(52),
        cost_estimate=cost(2 * clusters * near_count * leaf * leaf * cols, 24 << 20),
        name="near",
    )
    near = near_call(here, near_blocks, panel, from_chip, from_far)

    place = lax.axis_index(COL).astype(I32).reshape(1)
    return pl.pallas_call(
        functools.partial(final_kernel, rank, leaf),
        out_shape=jax.ShapeDtypeStruct((rows, cols), BF16),
        in_specs=[SMEM, VMEM, HBM, HBM],
        out_specs=HBM,
        scratch_shapes=[
            pltpu.VMEM((rank, rows), BF16),
            pltpu.VMEM((rows, cols), BF16),
            pltpu.VMEM((rows, cols), BF16),
            pltpu.SemaphoreType.DMA,
            pltpu.SemaphoreType.DMA((chunks // 2,)),
            pltpu.SemaphoreType.DMA((chunks // 2,)),
        ],
        compiler_params=params(52),
        cost_estimate=cost(4 * rows * rank * cols, 8 << 20),
        name="final",
    )(place, parts, row_basis.T, near)


def solution(mesh):
    devices = mesh.devices.reshape(2, 4, 4, 2, 2)
    fine = Mesh(devices, ("zl", "y", "x", "zh", "core"))
    placed = (
        P((*ROW, *COL), None),
        P(ROW, None),
        P((*ROW, *COL), None),
        P((*ROW, *COL), None, None, None),
        P(ROW, COL, None, None, None),
        P(ROW, COL, None),
        P(ROW, COL, None),
        P(ROW, COL),
    )
    return jax.shard_map(on_device, mesh=fine, in_specs=placed, out_specs=P((*ROW, *COL), None), check_vma=False)
```
